32 devices in a mesh: dp: 1 (over z), ep: 4 (over y), tp: 8 (over x, core).
Axes of the slice: x: 4, y: 4, z: 1, core: 2. Of those that a mesh axis runs over, the one named last changes fastest.
The devices are a block of a 4x4x8 slice.
Arguments:
- x: bfloat16 [512, 2048], P(('dp', 'ep'))
- idx: int32 [512, 8], P(('dp', 'ep'))
- g: float32 [512, 8], P(('dp', 'ep'))
- w1: bfloat16 [64, 2048, 1024], P('ep', None, 'tp')
- w3: bfloat16 [64, 2048, 1024], P('ep', None, 'tp')
- w2: bfloat16 [64, 1024, 2048], P('ep', 'tp')
Outputs:
- output: bfloat16 [512, 2048], P(('dp', 'ep'))
All inputs are finite; a program needn't handle non-finite values.
Results may differ from the reference program's by a relative error of at most 0.0100329.
Values are sent between devices in bfloat16 or wider.
A program may use at most 768 MiB of HBM per device.

```python
import jax
import jax.numpy as jnp
from jax import lax

D = 2048
F = 1024
E = 64
K = 8
TL = 128
EP = 4
CF = 2
C = CF * K * TL // E
T = EP * TL


def _weights(key, shape, fan_in):
    keys = jax.random.split(key, E)
    return lax.map(lambda k: (jax.random.normal(k, shape, jnp.float32) * fan_in ** -0.5).astype(jnp.bfloat16), keys)


def _draw_route(key, part):
    src_rank = jnp.arange(T, dtype=jnp.int32) // TL
    expert_ids = jnp.arange(E, dtype=jnp.int32)
    offset = (expert_ids[None, :] + 5 * src_rank[:, None] + 3 * part) % E
    rev_rank = (E - 1) - offset
    shift_q = rev_rank // 30
    remain = rev_rank % 30
    inv_weight = ((256 << shift_q) + ((256 << shift_q) * remain) // 30).astype(jnp.uint32)
    noise_bits = jax.random.bits(key, (T, E), jnp.uint32)
    lead_zero = jnp.zeros((T, E), jnp.uint32)
    for shift_n in range(32):
        lead_zero = lead_zero + (noise_bits < jnp.uint32(1 << (31 - shift_n))).astype(jnp.uint32)
    expo_int = lead_zero * 256 + (noise_bits & 255)
    wait_score = (expo_int * inv_weight) * E + expert_ids.astype(jnp.uint32)[None, :]
    return jnp.argsort(wait_score, axis=1)[:, :K].astype(jnp.int32)


def setup_inputs(seed: int = 0, part: int = 0) -> dict:
    kshared, kparts = jax.random.split(jax.random.key(seed))
    kx, ki, kg = jax.random.split(jax.random.fold_in(kparts, part), 3)
    k1, k3, k2 = jax.random.split(kshared, 3)
    x = jax.random.normal(kx, (T, D), jnp.float32).astype(jnp.bfloat16)
    idx = _draw_route(jax.random.fold_in(ki, 7), part)
    g = jax.nn.softmax(jax.random.normal(kg, (T, K), jnp.float32), axis=-1)
    w1 = _weights(k1, (D, F), D)
    w3 = _weights(k3, (D, F), D)
    w2 = _weights(k2, (F, D), F)
    return {"x": x, "idx": idx, "g": g, "w1": w1, "w3": w3, "w2": w2}


def _dest(idx_s):
    e = idx_s.reshape(-1)
    oh = jax.nn.one_hot(e, E, dtype=jnp.int32)
    slot = jnp.sum((jnp.cumsum(oh, axis=0) - oh) * oh, axis=1)
    return jnp.where(slot < C, e * C + slot, E * C)


def _expert(args):
    xe, a, b, c = args
    h1 = jnp.dot(xe, a, preferred_element_type=jnp.float32)
    h3 = jnp.dot(xe, b, preferred_element_type=jnp.float32)
    h = (jax.nn.silu(h1) * h3).astype(jnp.bfloat16)
    return jnp.dot(h, c, preferred_element_type=jnp.float32).astype(jnp.bfloat16)


def reference(x, idx, g, w1, w3, w2):
    dest = jax.vmap(_dest)(idx.reshape(EP, TL, K))
    xr = jnp.repeat(x.reshape(EP, TL, D), K, axis=1)
    buf = jax.vmap(lambda a, d: jnp.zeros((E * C, D), a.dtype).at[d].set(a, mode="drop"))(xr, dest)
    xe = buf.reshape(EP, E, C, D).transpose(1, 0, 2, 3).reshape(E, EP * C, D)
    ye = lax.map(_expert, (xe, w1, w3, w2))
    yb = ye.reshape(E, EP, C, D).transpose(1, 0, 2, 3).reshape(EP, E * C, D)
    yc = jax.vmap(lambda a, d: jnp.take(a, d, axis=0, mode="fill", fill_value=0))(yb, dest)
    out = jnp.sum(yc.reshape(EP, TL, K, D).astype(jnp.float32) * g.reshape(EP, TL, K, 1), axis=2)
    return out.reshape(T, D).astype(jnp.bfloat16)
```

```python
import functools

import jax
import jax.numpy as jnp
from jax import lax
from jax.experimental import pallas as pl
from jax.experimental.pallas import tpu as pltpu
from jax.sharding import PartitionSpec as P

CF = 2
BF = jnp.bfloat16
F32 = jnp.float32
MESH = pl.DeviceIdType.MESH
CW = 256
HG = 4


def _kernel(
    cap, x_hbm, tab_ref, w1, w3, w2, out_hbm,
    xall, tabs, w13, w2p, pm, xe, hp, cm, ych, z, b1, b2, s1, s2, ob,
    lx, lw, lw2, w2s, w2r, ts, tr, xs, xr, fs, fr, hs, hr, zs, zr, gs, gr, ks, kr, os_,
):
    TL, D = x_hbm.shape
    EL, _, FL = w1.shape
    NC = z.shape[0]
    DH = D // 2
    NX = z.shape[2]
    TQ = TL // NX
    q = lax.axis_index("ep")
    p = lax.axis_index("tp")
    x, c = p // 2, p % 2

    def ydev(k):
        return {"ep": (q + k) % 4}

    def xdev(k):
        return {"tp": ((x + k) % 4) * 2 + c}

    partner = {"tp": x * 2 + 1 - c}
    unsent = []

    def rc(src, dst, ss, rs, dev):
        return pltpu.make_async_remote_copy(
            src_ref=src, dst_ref=dst, send_sem=ss, recv_sem=rs, device_id=dev, device_id_type=MESH
        )

    def go(*a):
        cp = rc(*a)
        cp.start()
        unsent.append(cp)
        return cp

    cx = pltpu.make_async_copy(x_hbm, xall.at[0], lx)
    cx.start()

    def w13_copies(e):
        return (
            pltpu.make_async_copy(w1.at[e], w13.at[e, :, pl.ds(0, FL)], lw.at[0, e]),
            pltpu.make_async_copy(w3.at[e], w13.at[e, :, pl.ds(FL, FL)], lw.at[1, e]),
        )

    def start_w13(e, _):
        for cp in w13_copies(e):
            cp.start()
        return 0

    lax.fori_loop(0, EL, start_w13, 0)

    barrier = pltpu.get_barrier_semaphore()
    peers = [ydev(1), ydev(2), ydev(3), xdev(1), xdev(2), xdev(3), partner]
    for d in peers:
        pl.semaphore_signal(barrier, inc=1, device_id=d, device_id_type=MESH)
    tabs[0] = tab_ref[...]
    pl.semaphore_wait(barrier, len(peers))

    tcp = [go(tab_ref, tabs.at[4 - k], ts.at[k - 1], tr.at[k - 1], ydev(k)) for k in (1, 2, 3)]
    cx.wait()
    XR = TL // 4

    def rows(k):
        return pl.ds(pl.multiple_of(c * (2 * XR) + k * XR, XR), XR)

    def xl(src, dst, k, n, dev):
        return go(xall.at[src, rows(k)], xall.at[dst, rows(k)], xs.at[n], xr.at[n], dev)

    def fw(i, k):
        n = (i - 1) * 2 + k
        return go(xall.at[i, rows(k)], xall.at[i, rows(k)], fs.at[n], fr.at[n], partner)

    r0 = xl(0, 3, 0, 0, ydev(1))
    l1 = xl(0, 1, 1, 1, ydev(3))
    r1 = xl(0, 3, 1, 2, ydev(1))
    l0 = xl(0, 1, 0, 3, ydev(3))

    mine = pl.ds(pl.multiple_of(c * DH, DH), DH)
    theirs = pl.ds(pl.multiple_of((1 - c) * DH, DH), DH)
    cw2 = pltpu.make_async_copy(w2.at[:, :, mine], w2p.at[:, pl.ds(0, FL), :], lw2)
    cw2.start()
    rw2 = go(w2.at[:, :, theirs], w2p.at[:, pl.ds(FL, FL), :], w2s, w2r, partner)

    def route(i):
        idxf = tabs[i, 0:8, :]
        gg = tabs[i, 8:16, :]
        eid = (lax.broadcasted_iota(jnp.int32, (EL, TL), 0) + q * EL).astype(F32)
        m = jnp.zeros((EL, TL), F32)
        gt = jnp.zeros((EL, TL), F32)
        for j in range(8):
            eq = idxf[j : j + 1, :] == eid
            m = m + jnp.where(eq, 1.0, 0.0)
            gt = gt + jnp.where(eq, gg[j : j + 1, :], 0.0)
        tri = jnp.where(
            lax.broadcasted_iota(jnp.int32, (TL, TL), 0) < lax.broadcasted_iota(jnp.int32, (TL, TL), 1), 1.0, 0.0
        ).astype(BF)
        slot = jnp.dot(m.astype(BF), tri, preferred_element_type=F32)
        slot = jnp.where(m > 0.0, slot, -1.0)
        sid = lax.broadcasted_iota(jnp.int32, (cap, TL), 0).astype(F32)
        pgs = []
        for e in range(EL):
            hit = slot[e : e + 1, :] == sid
            pm[e * cap : (e + 1) * cap, :] = jnp.where(hit, 1.0, 0.0).astype(BF)
            pgs.append(jnp.where(hit, gt[e : e + 1, :], 0.0))
        pgt = jnp.concatenate(pgs, axis=0).T
        hi = pgt.astype(BF)
        rest = pgt - hi.astype(F32)
        mid = rest.astype(BF)
        lo = (rest - mid.astype(F32)).astype(BF)
        cm[i, 0:TL, :] = hi
        cm[i, TL : 2 * TL, :] = mid
        cm[i, 2 * TL : 3 * TL, :] = lo

    def gather(i):
        W = 512

        def step(n, _):
            cols = pl.ds(pl.multiple_of(n * W, W), W)
            r = jnp.dot(pm[...], xall[i, :, cols], preferred_element_type=F32)
            xe[:, i, :, cols] = r.astype(BF).reshape(EL, cap, W)
            return 0

        lax.fori_loop(0, D // W, step, 0)

    route(0)
    gather(0)
    r0.wait_recv()
    rr = xl(3, 2, 0, 4, ydev(1))
    f30 = fw(3, 0)
    l1.wait_recv()
    ll = xl(1, 2, 1, 5, ydev(3))
    f11 = fw(1, 1)
    r1.wait_recv()
    f31 = fw(3, 1)
    l0.wait_recv()
    f10 = fw(1, 0)
    for cp in tcp:
        cp.wait_recv()
    f30.wait_recv()
    f31.wait_recv()
    route(3)
    gather(3)
    f10.wait_recv()
    f11.wait_recv()
    route(1)
    gather(1)
    rr.wait_recv()
    f20 = fw(2, 0)
    ll.wait_recv()
    f21 = fw(2, 1)
    f20.wait_recv()
    f21.wait_recv()
    route(2)
    gather(2)

    def expert(e, _):
        for cp in w13_copies(e):
            cp.wait()
        ab = jnp.dot(xe[e].reshape(4 * cap, D), w13[e], preferred_element_type=F32)
        a, b = ab[:, :FL], ab[:, FL:]
        hp[e, :, 0:FL] = (jax.nn.silu(a) * b).astype(BF)
        return 0

    GE = EL // HG
    hcp = []
    for k in range(HG):
        lax.fori_loop(k * GE, (k + 1) * GE, expert, 0)
        es = pl.ds(k * GE, GE)
        hcp.append(
            go(hp.at[es, :, pl.ds(0, FL)], hp.at[es, :, pl.ds(FL, FL)], hs.at[k], hr.at[k], partner)
        )
    cw2.wait()
    rw2.wait_recv()
    for cp in hcp:
        cp.wait_recv()

    def compute(n):
        def ex(e, _):
            y = jnp.dot(hp[e], w2p[e, :, n * CW : (n + 1) * CW], preferred_element_type=F32)
            ych[:, pl.ds(pl.multiple_of(e * cap, cap), cap), :] = y.astype(BF).reshape(4, cap, CW)
            return 0

        lax.fori_loop(0, EL, ex, 0, unroll=4)

        def comb(i, _):
            t = jnp.dot(cm[i], ych[i], preferred_element_type=F32)
            t = t[0:TL] + t[TL : 2 * TL] + t[2 * TL : 3 * TL]
            z[n, i] = t.reshape(NX, TQ, CW)
            return 0

        lax.fori_loop(0, 4, comb, 0)

    def xi(k):
        return (x + k) % 4

    HQ = TQ // 2

    def big(n, yfirst):
        if yfirst:
            dev = ydev
            full = lambda k: z.at[n, k]
            half = lambda k, h: z.at[n, k, pl.ds(2 * h, 2)]
        else:
            dev = xdev
            full = lambda k: z.at[n, :, xi(k)]
            half = lambda k, h: z.at[n, pl.ds(2 * h, 2), xi(k)]
        return dev, full, half

    def small(n, yfirst):
        if yfirst:
            dev = xdev
            full = lambda k: z.at[n, 0, xi(k)]
            half = lambda k, h: z.at[n, 0, xi(k), pl.ds(h * HQ, HQ)]
        else:
            dev = ydev
            full = lambda k: z.at[n, k, x]
            half = lambda k, h: z.at[n, k, x, pl.ds(h * HQ, HQ)]
        return dev, full, half

    def opp(n, views, buf, step):
        dev, full, half = views
        return [
            go(half(2, 0), buf.at[n, 0], zs.at[n, step, 0], zr.at[n, step, 0], dev(1)),
            go(half(2, 1), buf.at[n, 1], zs.at[n, step, 1], zr.at[n, step, 1], dev(3)),
        ]

    def adj(n, views, cps, inbuf, buf, step):
        dev, full, half = views
        cps[0].wait_recv()
        r = half(1, 0)
        r[...] = r[...] + inbuf[n, 0]
        a = go(full(1), buf.at[n, 0], zs.at[n, step, 0], zr.at[n, step, 0], dev(1))
        cps[1].wait_recv()
        r = half(3, 1)
        r[...] = r[...] + inbuf[n, 1]
        b = go(full(3), buf.at[n, 1], zs.at[n, step, 1], zr.at[n, step, 1], dev(3))
        return [a, b]

    def fin(n, views, cps, inbuf):
        full = views[1]
        for cp in cps:
            cp.wait_recv()
        return full(0)[...] + inbuf[n, 0] + inbuf[n, 1]

    def ocols(n, cc):
        return pl.ds(pl.multiple_of(cc * DH + n * CW, CW), CW)

    def orows(k):
        return pl.ds(pl.multiple_of(xi(k) * TQ, TQ), TQ)

    st = {}

    def stage(s, n):
        yf = n % 2 == 0
        if s == 0:
            compute(n)
            st[n] = opp(n, big(n, yf), b1, 0)
        elif s == 1:
            st[n] = adj(n, big(n, yf), st[n], b1, b2, 1)
        elif s == 2:
            v = big(n, yf)
            r = v[1](0)
            r[...] = fin(n, v, st[n], b2)
            st[n] = opp(n, small(n, yf), s1, 2)
        elif s == 3:
            st[n] = adj(n, small(n, yf), st[n], s1, s2, 3)
        elif s == 4:
            o = fin(n, small(n, yf), st[n], s2)
            ob[orows(0), ocols(n, c)] = o.astype(BF)
            piece = ob.at[orows(0), ocols(n, c)]
            st[n] = [go(piece, piece, gs.at[n, k - 1], gr.at[n, k - 1], xdev(k)) for k in (2, 1, 3)]
            st[n].append(go(piece, piece, ks.at[n, 0], kr.at[n, 0], partner))
        elif s == 5:
            got = [st[n][3]]
            for k, cp in ((1, st[n][1]), (3, st[n][2]), (2, st[n][0])):
                cp.wait_recv()
                piece = ob.at[orows(4 - k), ocols(n, c)]
                got.append(go(piece, piece, ks.at[n, k], kr.at[n, k], partner))
            st[n] = got
        else:
            for cp in st[n]:
                cp.wait_recv()
            outs = []
            for cc in range(2):
                cols = pl.ds(cc * DH + n * CW, CW)
                cp = pltpu.make_async_copy(ob.at[:, cols], out_hbm.at[:, cols], os_.at[n, cc])
                cp.start()
                outs.append(cp)
            st[n] = outs

    for t in range(NC + 6):
        for s in range(7):
            if 0 <= t - s < NC:
                stage(s, t - s)
    for cp in unsent:
        cp.wait_send()
    for n in range(NC):
        for cp in st[n]:
            cp.wait()


def solution(mesh):
    nep, ntp = mesh.shape["ep"], mesh.shape["tp"]
    assert nep == 4 and ntp == 8
    tok = P(("dp", "ep"), None)

    def body(x, idx, g, w1, w3, w2):
        TL, D = x.shape
        K = idx.shape[1]
        EL, _, FL = w1.shape
        cap = CF * K * TL // (EL * nep)
        DH = D // 2
        NC = DH // CW
        NX = ntp // 2
        TQ = TL // NX
        tab = jnp.concatenate([idx.T.astype(F32), g.T], axis=0)
        dma = pltpu.SemaphoreType.DMA
        hbm = pl.BlockSpec(memory_space=pl.ANY)
        return pl.pallas_call(
            functools.partial(_kernel, cap),
            out_shape=jax.ShapeDtypeStruct((TL, D), BF),
            in_specs=[hbm, pl.BlockSpec(memory_space=pltpu.VMEM), hbm, hbm, hbm],
            out_specs=hbm,
            scratch_shapes=[
                pltpu.VMEM((nep, TL, D), BF),
                pltpu.VMEM((nep, 2 * K, TL), F32),
                pltpu.VMEM((EL, D, 2 * FL), BF),
                pltpu.VMEM((EL, 2 * FL, DH), BF),
                pltpu.VMEM((EL * cap, TL), BF),
                pltpu.VMEM((EL, nep, cap, D), BF),
                pltpu.VMEM((EL, nep * cap, 2 * FL), BF),
                pltpu.VMEM((nep, 3 * TL, EL * cap), BF),
                pltpu.VMEM((nep, EL * cap, CW), BF),
                pltpu.VMEM((NC, nep, NX, TQ, CW), F32),
                pltpu.VMEM((NC, 2, 2, TQ, CW), F32),
                pltpu.VMEM((NC, 2, 4, TQ, CW), F32),
                pltpu.VMEM((NC, 2, TQ // 2, CW), F32),
                pltpu.VMEM((NC, 2, TQ, CW), F32),
                pltpu.VMEM((TL, D), BF),
                dma, dma((2, EL)), dma, dma, dma,
                dma((3,)), dma((3,)), dma((6,)), dma((6,)), dma((6,)), dma((6,)),
                dma((HG,)), dma((HG,)), dma((NC, 4, 2)), dma((NC, 4, 2)),
                dma((NC, 3)), dma((NC, 3)), dma((NC, 4)), dma((NC, 4)), dma((NC, 2)),
            ],
            compiler_params=pltpu.CompilerParams(
                collective_id=0, has_side_effects=True, vmem_limit_bytes=60 * 1024 * 1024
            ),
        )(x, tab, w1, w3, w2)

    return jax.shard_map(
        body,
        mesh=mesh,
        in_specs=(tok, tok, tok, P("ep", None, "tp"), P("ep", None, "tp"), P("ep", "tp", None)),
        out_specs=tok,
        check_vma=False,
    )
```

```python
import functools

import jax
import jax.numpy as jnp
from jax import lax
from jax.experimental import pallas as pl
from jax.experimental.pallas import tpu as pltpu
from jax.sharding import PartitionSpec as P

CF = 2
BF = jnp.bfloat16
F32 = jnp.float32
MESH = pl.DeviceIdType.MESH
CW = 128
YW = 256
LG = 4
HSPLIT = (12, 4)


def _kernel(
    cap, x_hbm, idx_hbm, g_hbm, w1, w3, w2, out_ref,
    xall, itab, gtab, w13, w2p, pm, xe, hp, cm, ych, z, b1, b2, sm, ob,
    lx, li, lg, lw, lw2, ws, wr, its, itr, gts, gtr, xs, xr, fr, hs, hr, zs, zr, gs, gr, kr,
):
    TL, D = x_hbm.shape
    EL, _, FL = w1.shape
    NC = z.shape[0]
    DH = D // 2
    NX = z.shape[2]
    TQ = TL // NX
    K = idx_hbm.shape[0]
    sc = jax.named_scope
    q = lax.axis_index("ep")
    p = lax.axis_index("tp")
    x, c = p // 2, p % 2

    def ydev(k):
        return {"ep": (q + k) % 4}

    def xdev(k):
        return {"tp": ((x + k) % 4) * 2 + c}

    partner = {"tp": x * 2 + 1 - c}

    def go(src, dst, ss, rs, dev):
        cp = pltpu.make_async_remote_copy(
            src_ref=src, dst_ref=dst, send_sem=ss, recv_sem=rs, device_id=dev, device_id_type=MESH
        )
        cp.start()
        return cp

    def wait(sem, ref):
        pltpu.make_async_copy(ref, ref, sem).wait()

    cx = pltpu.make_async_copy(x_hbm, xall.at[0], lx)
    ci = pltpu.make_async_copy(idx_hbm, itab.at[0], li)
    cg = pltpu.make_async_copy(g_hbm, gtab.at[0], lg)
    for cp in (cx, ci, cg):
        cp.start()
    GL = EL // LG
    for k in range(LG):
        es = pl.ds(k * GL, GL)
        pltpu.make_async_copy(w1.at[es], w13.at[es, :, pl.ds(0, FL)], lw.at[k]).start()
        pltpu.make_async_copy(w3.at[es], w13.at[es, :, pl.ds(FL, FL)], lw.at[k]).start()
    mine = pl.ds(pl.multiple_of(c * DH, DH), DH)
    theirs = pl.ds(pl.multiple_of((1 - c) * DH, DH), DH)
    cw2 = pltpu.make_async_copy(w2.at[:, :, mine], w2p.at[:, pl.ds(0, FL), :], lw2)
    cw2.start()

    with sc("entry"):
        barrier = pltpu.get_barrier_semaphore()
        peers = [ydev(1), ydev(2), ydev(3), xdev(1), xdev(2), xdev(3), partner]
        for d in peers:
            pl.semaphore_signal(barrier, inc=1, device_id=d, device_id_type=MESH)
        for cp in (cx, ci, cg):
            cp.wait()
        pl.semaphore_wait(barrier, len(peers))

    XR = TL // 4

    def rows(k):
        return pl.ds(pl.multiple_of(c * (2 * XR) + k * XR, XR), XR)

    def xl(src, dst, k, n, dev):
        return go(xall.at[src, rows(k)], xall.at[dst, rows(k)], xs, xr.at[n], dev)

    def fw(i, k):
        go(xall.at[i, rows(k)], xall.at[i, rows(k)], xs, fr.at[i - 1], partner)

    def fwait(i):
        wait(fr.at[i - 1], xall.at[i, pl.ds(0, 2 * XR)])

    r0 = xl(0, 3, 0, 0, ydev(1))
    l1 = xl(0, 1, 1, 1, ydev(3))
    for k in (1, 3, 2):
        go(itab.at[0], itab.at[4 - k], its, itr, ydev(k))
        go(gtab.at[0], gtab.at[4 - k], gts, gtr, ydev(k))
    r1 = xl(0, 3, 1, 2, ydev(1))
    l0 = xl(0, 1, 0, 3, ydev(3))

    EH = EL // 2

    def swap_w2(k):
        es = pl.ds(k * EH, EH)
        go(w2.at[es, :, theirs], w2p.at[es, pl.ds(FL, FL), :], ws, wr, partner)

    swap_w2(0)

    def route(i):
        idx = itab[i]
        gg = gtab[i]
        eid = lax.broadcasted_iota(jnp.int32, (EL, TL), 0) + q * EL
        m = jnp.zeros((EL, TL), F32)
        gt = jnp.zeros((EL, TL), F32)
        for j in range(K):
            eq = idx[j : j + 1, :] == eid
            m = m + jnp.where(eq, 1.0, 0.0)
            gt = gt + jnp.where(eq, gg[j : j + 1, :], 0.0)
        tri = jnp.where(
            lax.broadcasted_iota(jnp.int32, (TL, TL), 0) < lax.broadcasted_iota(jnp.int32, (TL, TL), 1), 1.0, 0.0
        ).astype(BF)
        slot = jnp.dot(m.astype(BF), tri, preferred_element_type=F32)
        slot = jnp.where(m > 0.0, slot, -1.0)
        sid = lax.broadcasted_iota(jnp.int32, (cap, TL), 0).astype(F32)
        pgs = []
        for e in range(EL):
            hit = slot[e : e + 1, :] == sid
            pm[i, e * cap : (e + 1) * cap, :] = jnp.where(hit, 1.0, 0.0).astype(BF)
            pgs.append(jnp.where(hit, gt[e : e + 1, :], 0.0))
        pgt = jnp.concatenate(pgs, axis=0).T
        hi = pgt.astype(BF)
        rest = pgt - hi.astype(F32)
        mid = rest.astype(BF)
        lo = (rest - mid.astype(F32)).astype(BF)
        cm[i, 0:TL, :] = hi
        cm[i, TL : 2 * TL, :] = mid
        cm[i, 2 * TL : 3 * TL, :] = lo

    def gather(i):
        W = 512
        for n in range(D // W):
            cols = slice(n * W, (n + 1) * W)
            r = jnp.dot(pm[i], xall[i, :, cols], preferred_element_type=F32)
            xe[:, i, :, cols] = r.astype(BF).reshape(EL, cap, W)

    with sc("rg0"):
        route(0)
        gather(0)
    with sc("wait_tab"):
        wait(itr, itab.at[pl.ds(1, 3)])
        wait(gtr, gtab.at[pl.ds(1, 3)])
    with sc("routes"):
        for i in (3, 1, 2):
            route(i)
    with sc("wait_adj0"):
        r0.wait_recv()
        rr = xl(3, 2, 0, 4, ydev(1))
        fw(3, 0)
        l1.wait_recv()
        ll = xl(1, 2, 1, 5, ydev(3))
        fw(1, 1)
    with sc("wait_adj1"):
        r1.wait_recv()
        fw(3, 1)
        l0.wait_recv()
        fw(1, 0)
        swap_w2(1)
    with sc("wait_f3"):
        fwait(3)
    with sc("gather3"):
        gather(3)
    fwait(1)
    with sc("gather1"):
        gather(1)
    with sc("wait_opp"):
        rr.wait_recv()
        fw(2, 0)
        ll.wait_recv()
        fw(2, 1)
    with sc("wait_w13"):
        for k in range(LG):
            wait(lw.at[k], w13.at[pl.ds(k * GL, GL)])
    with sc("wait_opp2"):
        fwait(2)
    with sc("gather2"):
        gather(2)

    def expert(e):
        ab = jnp.dot(xe[e].reshape(4 * cap, D), w13[e], preferred_element_type=F32)
        a, b = ab[:, :FL], ab[:, FL:]
        hp[e, :, 0:FL] = (jax.nn.silu(a) * b).astype(BF)

    e0 = 0
    hgroups = []
    for k, ne in enumerate(HSPLIT):
        with sc(f"exp{k}"):
            for e in range(e0, e0 + ne):
                expert(e)
        es = pl.ds(e0, ne)
        hgroups.append(
            (e0, ne, go(hp.at[es, :, pl.ds(0, FL)], hp.at[es, :, pl.ds(FL, FL)], hs, hr.at[k], partner))
        )
        e0 += ne
    with sc("wait_w2"):
        cw2.wait()
        wait(wr, w2p.at[:, pl.ds(0, FL), :])

    PER = YW // CW

    def compute(n):
        cols = slice(n * YW, (n + 1) * YW)
        for e0, ne, cp in hgroups:
            if n == 0:
                with sc("wait_h"):
                    cp.wait_recv()
            with sc("ex"):
                for e in range(e0, e0 + ne):
                    y = jnp.dot(hp[e], w2p[e, :, cols], preferred_element_type=F32)
                    ych[:, e * cap : (e + 1) * cap, :] = y.astype(BF).reshape(4, cap, YW)
        with sc("comb"):
            for i in range(4):
                t = jnp.dot(cm[i], ych[i], preferred_element_type=F32)
                t = t[0:TL] + t[TL : 2 * TL] + t[2 * TL : 3 * TL]
                for k in range(PER):
                    z[n * PER + k, i] = t[:, k * CW : (k + 1) * CW].reshape(NX, TQ, CW)

    def xi(k):
        return (x + k) % 4

    def big(n):
        if n % 2 == 0:
            return ydev, lambda k: z.at[n, k], lambda k, h: z.at[n, k, pl.ds(2 * h, 2)]
        return xdev, lambda k: z.at[n, :, xi(k)], lambda k, h: z.at[n, pl.ds(2 * h, 2), xi(k)]

    def small(n):
        if n % 2 == 0:
            return xdev, lambda k: z.at[n, 0, xi(k)]
        return ydev, lambda k: z.at[n, k, x]

    def s0(n):
        dev, _, half = big(n)
        go(half(2, 0), b1.at[n, 0], zs, zr.at[n, 0], dev(1))
        go(half(2, 1), b1.at[n, 1], zs, zr.at[n, 0], dev(3))

    def s1(n):
        dev, full, half = big(n)
        wait(zr.at[n, 0], b1.at[n])
        r = half(1, 0)
        r[...] = r[...] + b1[n, 0]
        go(full(1), b2.at[n, 0], zs, zr.at[n, 1], dev(1))
        r = half(3, 1)
        r[...] = r[...] + b1[n, 1]
        go(full(3), b2.at[n, 1], zs, zr.at[n, 1], dev(3))

    def s2(n):
        wait(zr.at[n, 1], b2.at[n])
        r = big(n)[1](0)
        r[...] = r[...] + b2[n, 0] + b2[n, 1]
        dev, full = small(n)
        for k in (2, 1, 3):
            go(full(k), sm.at[n, k - 1], zs, zr.at[n, 2], dev(k))

    def ocols(m, cc):
        return pl.ds(pl.multiple_of(cc * DH + m * YW, YW), YW)

    def orows(k):
        return pl.ds(pl.multiple_of(xi(k) * TQ, TQ), TQ)

    def s3(m):
        parts = []
        for n in range(m * PER, (m + 1) * PER):
            wait(zr.at[n, 2], sm.at[n])
            parts.append(small(n)[1](0)[...] + sm[n, 0] + sm[n, 1] + sm[n, 2])
        ob[orows(0), ocols(m, c)] = jnp.concatenate(parts, axis=1).astype(BF)
        piece = ob.at[orows(0), ocols(m, c)]
        for k in (2, 1, 3):
            go(piece, piece, gs, gr.at[m], xdev(k))
        go(piece, piece, gs, kr.at[m], partner)

    def s4(m):
        wait(gr.at[m], ob.at[pl.ds(0, 3 * TQ), pl.ds(0, YW)])
        for k in (1, 2, 3):
            piece = ob.at[orows(k), ocols(m, c)]
            go(piece, piece, gs, kr.at[m], partner)

    def s5(m):
        wait(kr.at[m], ob.at[:, pl.ds(0, YW)])

    NM = NC // PER

    def per(f):
        def run(m):
            for n in range(m * PER, (m + 1) * PER):
                f(n)

        return run

    def first(m):
        compute(m)
        per(s0)(m)

    stages = [first, per(s1), per(s2), s3, s4, s5]
    order = [(0, 0), (0, 1), (0, 2), (1, 0), (0, 3), (1, 1), (2, 0), (1, 2), (2, 1), (1, 3)]
    order += [(3, 0), (2, 2), (3, 1), (2, 3), (4, 0), (3, 2), (4, 1), (3, 3), (4, 2), (4, 3)]
    order += [(5, m) for m in range(NM)]
    for s, m in order:
        with sc(f"st{s}_{m}"):
            stages[s](m)

    with sc("end"):
        out_ref[...] = ob[...]
        wait(its, itab.at[pl.ds(1, 3)])
        wait(gts, gtab.at[pl.ds(1, 3)])
        wait(xs, xe.at[pl.ds(0, 12), 0])
        wait(ws, w2p.at[:, pl.ds(0, FL), :])
        wait(hs, hp.at[:, :, pl.ds(0, FL)])
        wait(zs, xe.at[pl.ds(0, 15), 0])
        wait(gs, ob.at[pl.ds(0, TL * 7 // 8)])


def solution(mesh):
    nep, ntp = mesh.shape["ep"], mesh.shape["tp"]
    assert nep == 4 and ntp == 8
    tok = P(("dp", "ep"), None)

    def body(x, idx, g, w1, w3, w2):
        TL, D = x.shape
        K = idx.shape[1]
        EL, _, FL = w1.shape
        cap = CF * K * TL // (EL * nep)
        DH = D // 2
        NC = DH // CW
        NM = DH // YW
        NX = ntp // 2
        TQ = TL // NX
        assert TL // 4 == cap and NC * 15 * TQ * CW * 2 == 15 * cap * D
        dma = pltpu.SemaphoreType.DMA
        hbm = pl.BlockSpec(memory_space=pl.ANY)
        vmem = pl.BlockSpec(memory_space=pltpu.VMEM)
        return pl.pallas_call(
            functools.partial(_kernel, cap),
            out_shape=pltpu.VMEM((TL, D), BF),
            in_specs=[hbm] * 6,
            out_specs=vmem,
            scratch_shapes=[
                pltpu.VMEM((nep, TL, D), BF),
                pltpu.VMEM((nep, K, TL), jnp.int32),
                pltpu.VMEM((nep, K, TL), F32),
                pltpu.VMEM((EL, D, 2 * FL), BF),
                pltpu.VMEM((EL, 2 * FL, DH), BF),
                pltpu.VMEM((nep, EL * cap, TL), BF),
                pltpu.VMEM((EL, nep, cap, D), BF),
                pltpu.VMEM((EL, nep * cap, 2 * FL), BF),
                pltpu.VMEM((nep, 3 * TL, EL * cap), BF),
                pltpu.VMEM((nep, EL * cap, YW), BF),
                pltpu.VMEM((NC, nep, NX, TQ, CW), F32),
                pltpu.VMEM((NC, 2, 2, TQ, CW), F32),
                pltpu.VMEM((NC, 2, 4, TQ, CW), F32),
                pltpu.VMEM((NC, 3, TQ, CW), F32),
                pltpu.VMEM((TL, D), BF),
                dma, dma, dma, dma((LG,)), dma, dma, dma,
                dma, dma, dma, dma,
                dma, dma((6,)), dma((3,)),
                dma, dma((len(HSPLIT),)), dma, dma((NC, 3)),
                dma, dma((NM,)), dma((NM,)),
            ],
            compiler_params=pltpu.CompilerParams(
                collective_id=0, has_side_effects=True, vmem_limit_bytes=60 * 1024 * 1024
            ),
        )(x, idx.T, g.T, w1, w3, w2)

    return jax.shard_map(
        body,
        mesh=mesh,
        in_specs=(tok, tok, tok, P("ep", None, "tp"), P("ep", None, "tp"), P("ep", "tp", None)),
        out_specs=tok,
        check_vma=False,
    )
```
